32 devices in a mesh: gx: 16 (over z, y, x), gy: 2 (over core).
Axes of the slice: x: 2, y: 2, z: 4, core: 2. Of those that a mesh axis runs over, the one named last changes fastest.
Arguments:
- residual: bfloat16 [16, 2, 2048, 384], P('gx', 'gy'), may hold values from -6 to 6
- local_inverse: bfloat16 [16, 2, 2048, 2048], P('gx', 'gy'), may hold values from -0.125 to 0.125
- primal_basis: bfloat16 [16, 2, 96, 2048], P('gx', 'gy'), may hold values from -0.125 to 0.125
- row_stiffness: bfloat16 [16, 2, 2048], P('gx', 'gy'), may hold values from 0.099609375 to 10
- face_sizes: int32 [16, 2, 4], P('gx', 'gy'), may hold values from 0 to 512, as said below
- primal_slots: int32 [16, 2, 96], P('gx', 'gy'), may hold values from 0 to 287
- block_inverse: float32 [16, 2, 32, 64], P('gx', 'gy'), may hold values from -1 to 3
- level_basis: float32 [16, 2, 32, 64], P('gx', 'gy'), may hold values from -0.15625 to 0.15625
- top_inverse: float32 [64, 64], replicated, may hold values from -1 to 3
Outputs:
- preconditioned: bfloat16 [16, 2, 2048, 384], P('gx', 'gy')
The draws below stay inside these ranges and needn't reach their ends.
Inputs may be any that keep to these rules, and one draw needn't show every extreme that they name: face_sizes[x, y, f] is equal on the two sides of a shared face, 0 on faces at the grid's edge, at least 128 elsewhere; the value 512 is reached.
All inputs are finite; a program needn't handle non-finite values.
Results may differ from the reference program's by a relative error of at most 0.008.
Values may be sent and summed in bfloat16 or wider, within the bound.
No kernel may reach another device: no remote copies, remote signals or barrier semaphores. Data moves between devices by JAX's collectives and lax.ppermute only.
A program may use at most 64 MiB of HBM per device.

```python
import math
import jax
import jax.numpy as jnp
from jax import lax

W = 2048
R = 384
P_SIZE = 96
CDEV = 32
L3 = 64
SUBX = 16
SUBY = 2
CBS = 64


def draw_face_sizes(key, part):
    face_rows = W // 4
    key_x = jax.random.fold_in(key, 11)
    key_y = jax.random.fold_in(key, 12)
    edges_x = jax.random.randint(key_x, (SUBX - 1, SUBY), face_rows // 4, face_rows + 1, dtype=jnp.int32)
    edges_x = edges_x.at[0, 0].set(face_rows)
    edges_y = jax.random.randint(key_y, (SUBX, SUBY - 1), face_rows // 4, face_rows + 1, dtype=jnp.int32)
    blank_x = jnp.zeros((1, SUBY), jnp.int32)
    blank_y = jnp.zeros((SUBX, 1), jnp.int32)
    lower_x = jnp.concatenate([blank_x, edges_x], axis=0)
    upper_x = jnp.concatenate([edges_x, blank_x], axis=0)
    lower_y = jnp.concatenate([blank_y, edges_y], axis=1)
    upper_y = jnp.concatenate([edges_y, blank_y], axis=1)
    return jnp.stack([lower_x, upper_x, lower_y, upper_y], axis=-1)


def noise_field(key, shape):
    return jnp.clip(jax.random.normal(key, shape, jnp.float32), -4.0, 4.0)


def draw_block_inverse(key, part):
    key_noise = jax.random.fold_in(key, 21)
    key_diag = jax.random.fold_in(key, 22)
    noise = noise_field(key_noise, (SUBX, SUBY, CDEV, CBS))
    diagonal = jnp.exp(jax.random.uniform(key_diag, (SUBX, SUBY, CDEV, 1), jnp.float32, -0.7, 0.7))
    target = jnp.arange(SUBY)[:, None] * CDEV + jnp.arange(CDEV)[None, :]
    on_diag = jnp.arange(CBS)[None, None, :] == target[:, :, None]
    return 0.5 * noise / math.sqrt(CBS) + jnp.where(on_diag[None], diagonal, 0.0)


def draw_top_inverse(key, part):
    key_noise = jax.random.fold_in(key, 31)
    key_diag = jax.random.fold_in(key, 32)
    noise = noise_field(key_noise, (L3, L3))
    diagonal = jnp.exp(jax.random.uniform(key_diag, (L3, 1), jnp.float32, -0.7, 0.7))
    on_diag = jnp.arange(L3)[:, None] == jnp.arange(L3)[None, :]
    return 0.5 * noise / math.sqrt(L3) + jnp.where(on_diag, diagonal, 0.0)


def with_ends(result, own_key, low, largest):
    longest = result.shape.index(max(result.shape))
    spots = []
    for shift in (0, 1):
        where = [jax.random.randint(jax.random.fold_in(own_key, axis), (), 0, length) for axis, length in enumerate(result.shape)]
        where[longest] = (where[longest] + shift) % result.shape[longest]
        spots.append(tuple(where))
    return result.at[spots[0]].set(low).at[spots[1]].set(largest)


def levels(own_key, shape, shards, least, high):
    def one(dim, blocks):
        draws = jax.random.uniform(jax.random.fold_in(jax.random.fold_in(own_key, 6), dim), (blocks,), jnp.float32, least / len(shards), high / len(shards))
        return jnp.repeat(jnp.exp(draws), shape[dim] // blocks).reshape((-1,) + (1,) * (len(shape) - dim - 1))

    loudness = one(*shards[0])
    for cut in shards[1:]:
        loudness = loudness * one(*cut)
    return loudness


def gaussian(key, dims, width, most, shards=(), kind=jnp.bfloat16):
    result = jax.random.normal(key, dims, jnp.float32) * width
    if len(shards) > 0:
        result = levels(key, dims, shards, -0.22, 0.18) * result
    return jnp.clip(result, min=-most, max=most).astype(kind)


def setup_inputs(seed: int = 0) -> dict:
    streams_of = jax.random.split(jax.random.key(seed), 10)
    residual = gaussian(streams_of[0], (SUBX, SUBY, W, R), 1.0, 6.0, ((0, 16), (1, 2)))
    local_inverse = gaussian(streams_of[1], (SUBX, SUBY, W, W), W ** -0.5, 0.125, ((0, 16), (1, 2)))
    primal_basis = gaussian(streams_of[2], (SUBX, SUBY, P_SIZE, W), W ** -0.5, 0.125, ((0, 16), (1, 2)))
    row_stiffness = jnp.clip(jnp.exp(math.log(10.0) - 4.609084 * jax.random.uniform(streams_of[3], (SUBX, SUBY, W), jnp.float32) ** levels(streams_of[3], (SUBX, SUBY, W), ((0, 16), (1, 2)), -0.2, 0.2)), 0.099609375, 10.0).astype(jnp.bfloat16)
    face_sizes = draw_face_sizes(jax.random.fold_in(streams_of[9], 71), 0)
    primal_slots = with_ends(jax.random.randint(streams_of[5], (SUBX, SUBY, P_SIZE), 0, 9 * CDEV), jax.random.fold_in(streams_of[5], 1), 0, (9 * CDEV) - 1).astype(jnp.int32)
    block_inverse = draw_block_inverse(jax.random.fold_in(streams_of[9], 71), 0)
    level_basis = gaussian(streams_of[7], (SUBX, SUBY, CDEV, L3), (48 * CDEV) ** -0.5, 0.15625, ((0, 16), (1, 2)), jnp.float32)
    top_inverse = draw_top_inverse(jax.random.fold_in(streams_of[9], 71), 0)
    return dict(residual=residual, local_inverse=local_inverse, primal_basis=primal_basis, row_stiffness=row_stiffness, face_sizes=face_sizes, primal_slots=primal_slots, block_inverse=block_inverse, level_basis=level_basis, top_inverse=top_inverse)


def partner_rows(values):
    face_rows = W // 4
    tail = values.shape[3:]
    parts = values.reshape((SUBX, SUBY, 4, face_rows) + tail)
    rest = [(0, 0)] * (len(tail) + 1)
    low_x = jnp.pad(parts[:, :, 1], [(1, 0), (0, 0)] + rest)[:SUBX]
    high_x = jnp.pad(parts[:, :, 0], [(0, 1), (0, 0)] + rest)[1:]
    low_y = jnp.pad(parts[:, :, 3], [(0, 0), (1, 0)] + rest)[:, :SUBY]
    high_y = jnp.pad(parts[:, :, 2], [(0, 0), (0, 1)] + rest)[:, 1:]
    return jnp.stack([low_x, high_x, low_y, high_y], axis=2).reshape(values.shape)


def reference(residual, local_inverse, primal_basis, row_stiffness, face_sizes, primal_slots, block_inverse, level_basis, top_inverse):
    highest = lax.Precision.HIGHEST
    face_rows = W // 4
    position = jnp.arange(W, dtype=jnp.int32)
    face_of_row = position // face_rows
    counts = face_sizes[:, :, face_of_row]
    live_rows = (position % face_rows)[None, None, :] < counts
    masked = jnp.where(live_rows[..., None], residual, jnp.zeros((), jnp.bfloat16))

    def local_solve(subdomain):
        inverse, own_rows, primal_phi = subdomain
        return (jnp.dot(inverse, own_rows, preferred_element_type=jnp.float32),
                jnp.dot(primal_phi, own_rows, preferred_element_type=jnp.float32))

    local_part, partial_value = lax.map(local_solve, (local_inverse.reshape(SUBX * SUBY, W, W),
                                                masked.reshape(SUBX * SUBY, W, R),
                                                primal_basis.reshape(SUBX * SUBY, P_SIZE, W)))
    local_part = local_part.reshape(SUBX, SUBY, W, R)
    partial_value = partial_value.reshape(SUBX, SUBY, P_SIZE, R)
    selector = (primal_slots[..., None] == jnp.arange(9 * CDEV, dtype=jnp.int32)).astype(jnp.float32)
    spread = jnp.einsum('xyps,xypr->xysr', selector, partial_value, precision=highest).reshape(SUBX, SUBY, 3, 3, CDEV, R)
    padded = jnp.pad(spread, ((1, 1), (1, 1), (0, 0), (0, 0), (0, 0), (0, 0)))
    assembled = jnp.zeros((SUBX, SUBY, CDEV, R), jnp.float32)
    for shift_x in range(3):
        for shift_y in range(3):
            assembled = assembled + padded[2 - shift_x:2 - shift_x + SUBX, 2 - shift_y:2 - shift_y + SUBY, shift_x, shift_y]
    block_rhs = assembled.reshape(SUBX, SUBY * CDEV, R)
    top_rhs = jnp.einsum('xycl,xycr->lr', level_basis, assembled, precision=highest)
    top_value = jnp.dot(top_inverse, top_rhs, precision=highest)
    coarse = jnp.einsum('xycs,xsr->xycr', block_inverse, block_rhs, precision=highest)
    coarse = coarse + jnp.einsum('xycl,lr->xycr', level_basis, top_value, precision=highest)
    coarse_pad = jnp.pad(coarse, ((1, 1), (1, 1), (0, 0), (0, 0)))
    beside_all = jnp.stack([coarse_pad[shift_x:shift_x + SUBX, shift_y:shift_y + SUBY]
                        for shift_x in range(3) for shift_y in range(3)], axis=2).reshape(SUBX, SUBY, 9 * CDEV, R)
    primal_values = jnp.einsum('xyps,xysr->xypr', selector, beside_all, precision=highest)
    stiffness = row_stiffness.astype(jnp.float32)
    coarse_rows = jnp.einsum('xypw,xypr->xywr', primal_basis.astype(jnp.float32), primal_values, precision=highest)
    sent = jnp.where(live_rows[..., None], stiffness[..., None] * local_part + stiffness[..., None] * coarse_rows, 0.0).astype(jnp.bfloat16)
    summed = sent.astype(jnp.float32) + partner_rows(sent).astype(jnp.float32)
    divisor = stiffness + partner_rows(row_stiffness).astype(jnp.float32)
    return jnp.where(live_rows[..., None], summed / divisor[..., None], 0.0).astype(jnp.bfloat16)
```

```python
import functools

import jax
import jax.numpy as jnp
from jax import lax
from jax.experimental import pallas as pl
from jax.experimental.pallas import tpu as pltpu
from jax.sharding import PartitionSpec as P

BF = jnp.bfloat16
F32 = jnp.float32
I32 = jnp.int32
INVERSE_LANE = 128
VMEM = pltpu.VMEM
SMEM = pltpu.SMEM


def near_pairs(count):
    return [(i, i ^ 1) for i in range(count) if i ^ 1 < count]


def far_pairs(count):
    return [(i, i + 1 if i % 2 else i - 1) for i in range(1, count) if i % 2 == 0 or i + 1 < count]


def swapped(block, axis, pairs):
    return lax.ppermute(block, axis, pairs) if pairs else jnp.zeros_like(block)


def dot(a, b):
    return jnp.dot(a.astype(BF), b.astype(BF), preferred_element_type=F32)


def tdot(a, b):
    return lax.dot_general(
        a.astype(BF), b.astype(BF), (((0,), (0,)), ((), ())), preferred_element_type=F32
    )


def whole(spaces):
    return [pl.BlockSpec(memory_space=space) for space in spaces]


def call(body, outs, inputs, flops=1 << 22):
    spaces = [SMEM] + [VMEM] * (len(inputs) - 1)
    return pl.pallas_call(
        body,
        out_shape=[jax.ShapeDtypeStruct(shape, kind) for shape, kind in outs],
        in_specs=whole(spaces),
        out_specs=whole([VMEM] * len(outs)),
        cost_estimate=pl.CostEstimate(flops=flops, bytes_accessed=1 << 20, transcendentals=0),
        compiler_params=pltpu.CompilerParams(vmem_limit_bytes=6 << 20),
    )(*inputs)


class Sizes:
    pass


def slot_row(block):
    rows = block.astype(F32)
    return (rows[0:1] * 16.0 + rows[1:2]).astype(I32)


def face_slice(ref, index, face):
    return ref[:, pl.ds(pl.multiple_of(index * face, 128), face)]


def pack_small(z, info, slots, level, inverse, out):
    out[0 : z.coarse, :] = jnp.zeros((z.coarse, z.span), BF)
    out[0 : z.coarse, 0 : z.top] = level[...].astype(BF)
    out[0 : z.coarse, INVERSE_LANE : INVERSE_LANE + z.block] = inverse[...].astype(BF)


def pack_marks(z, slots, stiff, out, base):
    row = lax.broadcasted_iota(I32, (16, z.span), 0)
    full = jnp.where(row == 2, stiff.astype(F32), 0.0)
    out[base : base + 16, :] = full.astype(BF)
    value = slots[...]
    high = lax.shift_right_logical(value, 4)
    low = value - high * 16
    row = lax.broadcasted_iota(I32, (16, z.primal), 0)
    marks = jnp.where(row == 0, high, jnp.where(row == 1, low, 0)).astype(F32)
    out[base : base + 16, 0 : z.primal] = jnp.where(row == 2, full[:, : z.primal], marks).astype(BF)


def pack_line(z, info, phi, stiff, slots, level, inverse, *outs):
    yodd = info[5] % 2
    pack_small(z, info, slots, level, inverse, outs[0])
    pack_marks(z, slots, face_slice(stiff, 3 - yodd, z.face), outs[0], z.coarse)
    base = z.coarse + 16
    outs[0][base : base + z.primal, :] = face_slice(phi, 3 - yodd, z.face)
    if len(outs) > 1:
        outs[1][0 : z.primal, :] = face_slice(phi, 2 + yodd, z.face)
        pack_marks(z, slots, face_slice(stiff, 2 + yodd, z.face), outs[1], z.primal)


def pack_sides(z, info, phi, stiff, slots, *refs):
    line, (to_a, to_b) = refs[:-2], refs[-2:]
    odd = info[4]
    to_a[0 : z.primal, :] = face_slice(phi, 1 - odd, z.face)
    pack_marks(z, slots, face_slice(stiff, 1 - odd, z.face), to_a, z.primal)
    base = z.primal + 16
    for y in range(z.ny):
        to_a[base + y * z.coarse : base + (y + 1) * z.coarse, :] = small_of(z, line, y)
    to_b[0 : z.primal, :] = face_slice(phi, odd, z.face)
    pack_marks(z, slots, face_slice(stiff, odd, z.face), to_b, z.primal)


def small_of(z, line, y):
    return line[y][0 : z.coarse, :] if z.paired else line[0][y, 0 : z.coarse, :]


def marks_of(z, line, y):
    if z.paired:
        return line[y][z.coarse : z.coarse + 16, 0 : z.primal]
    return line[0][y, z.coarse : z.coarse + 16, 0 : z.primal]


def row_of(z, slot, y, own_y, place):
    side_x = slot // (3 * z.coarse)
    rest = slot - side_x * (3 * z.coarse)
    side_y = rest // z.coarse
    target = y + side_y - 1
    order = (target + own_y) % 2 if z.paired else target
    row = place(side_x - 1) * z.line + order * z.coarse + rest - side_y * z.coarse
    return jnp.where((target >= 0) & (target < z.ny), row, -1)


def one_hot(rows, count):
    return (lax.broadcasted_iota(I32, (count, rows.shape[1]), 0) == rows).astype(F32).astype(BF)


def spread_body(z, info, *refs):
    line, partial, (to_b, to_a, middle) = refs[: z.lines], refs[z.lines : -3], refs[-3:]
    own_y = info[5]
    total = jnp.zeros((3 * z.line, z.vectors), F32)
    for y in range(z.ny):
        at = (own_y + y) % 2 if z.paired else y
        rows = row_of(z, slot_row(marks_of(z, line, y)), at, own_y, lambda side: side + 1)
        block = partial[y][...] if z.paired else partial[0][y]
        total += dot(one_hot(rows, 3 * z.line), block)
    down, up = total[: z.line], total[2 * z.line :]
    even = info[4] == 0
    to_b[...] = jnp.where(even, down, up).astype(BF)
    to_a[...] = jnp.where(even, up, down).astype(BF)
    middle[...] = total[z.line : 2 * z.line]


def level_line(z, line):
    return jnp.concatenate([small_of(z, line, y)[:, : z.top] for y in range(z.ny)], axis=0)


def top_body(z, info, *refs):
    line = refs[: z.lines]
    side_a, came, to_a, middle, message, top_part, kept = refs[z.lines :]
    value = middle[...] + came[...].astype(F32)
    base = z.primal + 16
    level_a = side_a[base : base + z.line, 0 : z.top]
    part = tdot(level_line(z, line), value) + tdot(level_a, to_a[...])
    top_part[...] = part
    kept[...] = value
    message[0 : z.top, :] = part.astype(BF)
    message[z.top : z.top + z.line, :] = to_a[...]
    message[z.top + z.line :, :] = value.astype(BF)


def coarse_body(z, info, *refs):
    line = refs[: z.lines]
    side_a, answer, top_part, kept, to_a, total, total_sent, beyond = refs[z.lines :]
    summed = top_part[...] + answer[0 : z.top, :].astype(F32)
    total[...] = summed
    total_sent[...] = summed.astype(BF)
    own = kept[...] + answer[z.top : z.top + z.line, :].astype(F32)
    other = to_a[...].astype(F32) + answer[z.top + z.line :, :].astype(F32)

    def ordered(block):
        if not z.paired:
            return block
        turned = jnp.concatenate([block[z.coarse :], block[: z.coarse]], axis=0)
        return jnp.where(info[5] == 0, block, turned)

    base = z.primal + 16
    beyond[0 : z.line, :] = dot(
        side_a[base : base + z.line, INVERSE_LANE : INVERSE_LANE + z.block], ordered(other)
    ).astype(BF)
    inverse = jnp.concatenate(
        [small_of(z, line, y)[:, INVERSE_LANE : INVERSE_LANE + z.block] for y in range(z.ny)], axis=0
    )
    beyond[z.line : 2 * z.line, :] = dot(inverse, ordered(own)).astype(BF)
    beyond[2 * z.line :, :] = jnp.zeros((z.line, z.vectors), BF)
    beyond[2 * z.line :, 0 : z.top] = level_line(z, line)
    beyond[2 * z.line :, INVERSE_LANE : INVERSE_LANE + z.top] = side_a[base : base + z.line, 0 : z.top]


def values_body(z, info, *refs):
    line = refs[: z.lines]
    side_a, side_b, beyond, come, over, top_inverse, near, top_map = refs[z.lines :]
    own_y = info[5]
    sign = 1 - 2 * info[4]
    first, second, third = slice(0, z.line), slice(z.line, 2 * z.line), slice(2 * z.line, 3 * z.line)
    late = slice(INVERSE_LANE, INVERSE_LANE + z.top)
    coarse = jnp.concatenate(
        [come[first], come[second], beyond[second], beyond[first], over[second]], axis=0
    )
    levels = jnp.concatenate(
        [
            come[third, late],
            come[third, 0 : z.top],
            beyond[third, 0 : z.top],
            beyond[third, late],
            over[third, 0 : z.top],
        ],
        axis=0,
    )
    levels = dot(levels, top_inverse[...])
    marks = slice(z.primal, z.primal + 16)
    wanted = [
        (None, own_y, 0),
        (side_a[marks, 0 : z.primal], own_y, 1),
        (side_b[marks, 0 : z.primal], own_y, -1),
    ]
    if z.paired:
        wanted[0] = (marks_of(z, line, 0), own_y, 0)
        wanted.append((marks_of(z, line, 1), 1 - own_y, 0))
    else:
        wanted[0] = (line[0][own_y, z.coarse : z.coarse + 16, 0 : z.primal], own_y, 0)
        yodd = own_y % 2
        for shift in (1 - 2 * yodd, 2 * yodd - 1):
            other = jnp.clip(own_y + shift, 0, z.ny - 1)
            wanted.append((line[0][other, z.coarse : z.coarse + 16, 0 : z.primal], other, 0))
    for i, (block, y, at) in enumerate(wanted):
        rows = row_of(z, slot_row(block), y, own_y, lambda side: sign * side + at + 2)
        chosen = one_hot(rows, 5 * z.line)
        near[i * z.primal : (i + 1) * z.primal, :] = tdot(chosen, coarse)
        top_map[i * z.primal : (i + 1) * z.primal, :] = tdot(chosen, levels).astype(BF)


def spread_column(row, count):
    high = row.astype(BF)
    low = (row - high.astype(F32)).astype(BF)
    at = lax.broadcasted_iota(I32, (16, row.shape[1]), 0)
    pair = jnp.where(at == 0, high.astype(F32), jnp.where(at == 1, low.astype(F32), 0.0))
    return tdot(pair, jnp.ones((16, count), F32))


def weighted_body(z, info, which, inverse, masked, stiff, out):
    value = dot(inverse[...], masked[...])
    out[...] = (value * spread_column(stiff[...].astype(F32), z.vectors)).astype(BF)


def weighted_face(z, inverse, masked, stiff, info, index):
    tiles = 2
    rows = z.face // tiles
    return pl.pallas_call(
        functools.partial(weighted_body, z),
        out_shape=jax.ShapeDtypeStruct((z.face, z.vectors), BF),
        grid_spec=pltpu.PrefetchScalarGridSpec(
            num_scalar_prefetch=2,
            grid=(tiles,),
            in_specs=[
                pl.BlockSpec((rows, z.rows), lambda i, info, which: (which[0] * tiles + i, 0)),
                pl.BlockSpec((z.rows, z.vectors), lambda i, info, which: (0, 0)),
                pl.BlockSpec((1, rows), lambda i, info, which: (0, which[0] * tiles + i)),
            ],
            out_specs=pl.BlockSpec((rows, z.vectors), lambda i, info, which: (i, 0)),
        ),
        cost_estimate=pl.CostEstimate(
            flops=2 * z.face * z.rows * z.vectors,
            bytes_accessed=2 * z.face * z.rows,
            transcendentals=0,
        ),
        compiler_params=pltpu.CompilerParams(vmem_limit_bytes=12 << 20),
    )(info, index, inverse, masked, stiff)


def final_body(z, info, order, phi, stiff, near, top_map, total, came, *refs):
    given, (out, values) = refs[:-2], refs[-2:]
    step = pl.program_id(0)

    @pl.when(step == 0)
    def _():
        top = total[...] + came[...].astype(F32)
        values[...] = (near[...] + dot(top_map[...], top)).astype(BF)

    for side in range(4):

        @pl.when(step == side)
        def _(side=side):
            own = given[side]
            stiff_row = stiff[...].astype(F32)
            value = own[...].astype(F32)
            value += tdot(phi[...].astype(F32) * stiff_row, values[0 : z.primal, :])
            scale = stiff_row
            if side < z.sides:
                got, static = given[4 + side], given[4 + z.sides + side]
                base = z.phi_base[side]
                mark = z.mark_base[side]
                other_row = static[mark : mark + 16, :].astype(F32)[2:3, :]
                value += got[...].astype(F32)
                value += tdot(
                    static[base : base + z.primal, :].astype(F32) * other_row,
                    values[(1 + side) * z.primal : (2 + side) * z.primal, :],
                )
                scale = scale + other_row
            value = value * spread_column(1.0 / scale, z.vectors)
            live = lax.broadcasted_iota(I32, value.shape, 0) < info[order[side]]
            out[...] = jnp.where(live, value, 0.0).astype(BF)


def local(
    residual,
    local_inverse,
    primal_basis,
    row_stiffness,
    face_sizes,
    primal_slots,
    block_inverse,
    level_basis,
    top_inverse,
):
    nx, ny = lax.axis_size("gx"), lax.axis_size("gy")
    odd = lax.axis_index("gx") % 2
    own_y = lax.axis_index("gy")
    yodd = own_y % 2
    near_x, far_x = near_pairs(nx), far_pairs(nx)
    near_y, far_y = near_pairs(ny), far_pairs(ny)

    z = Sizes()
    own_rows = residual[0, 0]
    phi = primal_basis[0, 0]
    stiff = row_stiffness[0]
    slots = primal_slots[0]
    z.ny, z.paired = ny, ny == 2
    z.rows, z.vectors = own_rows.shape
    z.face = z.rows // 4
    z.primal = phi.shape[0]
    z.coarse, z.block = block_inverse.shape[2:]
    z.top = level_basis.shape[3]
    z.line = ny * z.coarse
    z.lines = 2 if z.paired else 1
    z.span = z.face
    z.sides = 3 if z.paired else 4
    counts = face_sizes[0, 0]
    at = jnp.arange(8, dtype=I32)
    info = jnp.where(at == 4, odd, jnp.where(at == 5, own_y, jnp.pad(counts, (0, 4))))

    bound = functools.partial
    marked = z.coarse + 16
    outs = [((marked + z.primal, z.span), BF)]
    if far_y:
        outs.append(((z.primal + 16, z.span), BF))
    packed = call(
        bound(pack_line, z), outs, [info, phi, stiff, slots, level_basis[0, 0], block_inverse[0, 0]]
    )
    if z.paired:
        other = swapped(packed[0], "gy", near_y)
        line = [packed[0], other]
        y_static = [other]
        z.phi_base, z.mark_base = [0, 0, marked], [z.primal, z.primal, z.coarse]
    else:
        line = [lax.all_gather(packed[0][:marked], "gy", axis=0)]
        y_static = [swapped(packed[0], "gy", near_y)]
        z.phi_base, z.mark_base = [0, 0, marked, 0], [z.primal, z.primal, z.coarse, z.primal]
        y_static.append(swapped(packed[1], "gy", far_y) if far_y else jnp.zeros((z.primal + 16, z.span), BF))

    sent_a, sent_b = call(
        bound(pack_sides, z),
        [((z.primal + 16 + z.line, z.span), BF), ((z.primal + 16, z.span), BF)],
        [info, phi, stiff, slots] + line,
    )
    side_a = swapped(sent_a, "gx", near_x)
    side_b = swapped(sent_b, "gx", far_x)

    position = jnp.arange(z.rows, dtype=I32)
    picked = jnp.where(
        (position // z.face)[:, None] == jnp.arange(4, dtype=I32)[None, :], counts[None, :], 0
    )
    live = (position % z.face < jnp.sum(picked, axis=1))[:, None]
    masked = jnp.where(live, own_rows, jnp.zeros((), BF))
    partial = jnp.dot(phi, masked, preferred_element_type=F32).astype(BF)
    if z.paired:
        partial_line = [partial, swapped(partial, "gy", near_y)]
    else:
        partial_line = [lax.all_gather(partial, "gy", axis=0)]
    wide = (z.line, z.vectors)
    to_b, to_a, middle = call(
        bound(spread_body, z), [(wide, BF), (wide, BF), (wide, F32)], [info] + line + partial_line
    )
    came = swapped(to_b, "gx", far_x)
    message, top_part, kept = call(
        bound(top_body, z),
        [((z.top + 2 * z.line, z.vectors), BF), ((z.top, z.vectors), F32), (wide, F32)],
        [info] + line + [side_a, came, to_a, middle],
    )
    answer = swapped(message, "gx", near_x)
    total, total_sent, beyond = call(
        bound(coarse_body, z),
        [
            ((z.top, z.vectors), F32),
            ((z.top, z.vectors), BF),
            ((3 * z.line, z.vectors), BF),
        ],
        [info] + line + [side_a, answer, top_part, kept, to_a],
    )
    come = swapped(beyond, "gx", far_x)
    over = swapped(come, "gx", near_x)
    arrived = jnp.zeros((z.top, z.vectors), BF)
    step = 2
    while step < nx:
        if step > 2:
            total = total + arrived
            total_sent = total.astype(BF)
        arrived = lax.ppermute(total_sent, "gx", [(i, i ^ step) for i in range(nx)])
        step *= 2

    count = 1 + z.sides
    near, top_map = call(
        bound(values_body, z),
        [((count * z.primal, z.vectors), F32), ((count * z.primal, z.top), BF)],
        [info] + line + [side_a, side_b, beyond, come, over, top_inverse],
    )

    order = jnp.where(
        at == 0, 1 - odd, jnp.where(at == 1, odd, jnp.where(at == 2, 3 - yodd, 2 + yodd))
    )
    pairs = [("gx", near_x), ("gx", far_x), ("gy", near_y), ("gy", far_y)]
    own = [weighted_face(z, local_inverse[0, 0], masked, stiff, info, order[i : i + 1]) for i in range(4)]
    got = [swapped(own[i], *pairs[i]) for i in range(z.sides)]

    static = [side_a, side_b] + y_static
    fixed = lambda i, info, order: (0, 0)
    full = lambda item: pl.BlockSpec(item.shape, fixed)
    given = own + got + static
    result = pl.pallas_call(
        bound(final_body, z),
        out_shape=jax.ShapeDtypeStruct((z.rows, z.vectors), BF),
        grid_spec=pltpu.PrefetchScalarGridSpec(
            num_scalar_prefetch=2,
            grid=(4,),
            in_specs=[
                pl.BlockSpec((z.primal, z.face), lambda i, info, order: (0, order[i])),
                pl.BlockSpec((1, z.face), lambda i, info, order: (0, order[i])),
            ]
            + [full(item) for item in [near, top_map, total, arrived] + given],
            out_specs=pl.BlockSpec((z.face, z.vectors), lambda i, info, order: (order[i], 0)),
            scratch_shapes=[pltpu.VMEM((count * z.primal, z.vectors), BF)],
        ),
        cost_estimate=pl.CostEstimate(flops=1 << 30, bytes_accessed=1 << 22, transcendentals=0),
        compiler_params=pltpu.CompilerParams(vmem_limit_bytes=16 << 20),
    )(info, order, phi, stiff, near, top_map, total, arrived, *given)
    return result[None, None]


def solution(mesh):
    in_specs = (
        P("gx", "gy", None, None),
        P("gx", "gy", None, None),
        P("gx", "gy", None, None),
        P("gx", "gy", None),
        P("gx", "gy", None),
        P("gx", "gy", None),
        P("gx", "gy", None, None),
        P("gx", "gy", None, None),
        P(),
    )
    out_specs = P("gx", "gy", None, None)
    return jax.shard_map(local, mesh=mesh, in_specs=in_specs, out_specs=out_specs, check_vma=False)
```
